128 devices in a mesh: chain: 16 (over z, y_lo, core), tech: 4 (over x), blk: 2 (over y_hi).
Axes of the slice: x: 4, y: 4 (y_hi: 2, y_lo: 2; y = y_hi * 2 + y_lo), z: 4, core: 2. Of those that a mesh axis runs over, the one named last changes fastest.
Arguments:
- block_inverse: bfloat16 [4, 16, 3072, 3072], P('tech', 'chain', 'blk'), may hold values from -1 to 4.5, as said below
- coupling: bfloat16 [4, 16, 3072, 512], P('tech', 'chain', 'blk'), may hold values from -0.0390625 to 0.0390625
- data_rhs: bfloat16 [4, 16, 3072, 256], P('tech', 'chain', 'blk'), may hold values from -6 to 6
- station_seen: int32 [4, 16, 1024], P('tech', 'chain', 'blk'), may hold values 0 or 1
- shared_inverse: float32 [16, 512, 512], P('chain'), may hold values from -0.05 to 1, as said below
- walk_weight: float32 [512], replicated, may hold values from 0.92 to 1
- shared_rhs: float32 [16, 512, 256], P('chain'), may hold values from -1.2 to 1.2
Outputs:
- coords: float32 [4, 16, 3072, 256], P('tech', 'chain', 'blk')
- shared: float32 [16, 512, 256], P('chain')
The draws below stay inside these ranges and needn't reach their ends.
Inputs may be any that keep to these rules, and one draw needn't show every extreme that they name: `block_inverse`: each block is symmetric. `shared_inverse`: each block is symmetric.
All inputs are finite; a program needn't handle non-finite values. No bound on the sum of `station_seen` on one device may be relied on, other than what follows from the above.
Results may differ from the reference program's by a relative error of at most 0.004.
Values may be sent and summed in bfloat16 or wider, within the bound.
No kernel may reach another device: no remote copies, remote signals or barrier semaphores. Data moves between devices by JAX's collectives and lax.ppermute only.
A program may use at most 128 MiB of HBM per device.

```python
import math
import jax
import jax.numpy as jnp
from jax import lax

STATIONS = 1024
SHARED = 512
SAMPLES = 256
SWEEPS = 2
B = 3072
WEEKS = 16
GROUPS = 4


def symmetric_block(block_key, order, diag_low, diag_high, spread):
    first_key, second_key = jax.random.split(block_key)
    diagonal = jnp.exp(jax.random.uniform(first_key, (order,), jnp.float32, jnp.log(diag_low), jnp.log(diag_high)))
    noise = jax.random.normal(second_key, (order, order), jnp.float32)
    noise = jnp.clip((noise + noise.T) * 0.7071067811865476, -4.0, 4.0) * (spread / jnp.sqrt(1.0 * order))
    root = jnp.sqrt(diagonal)
    return jnp.diag(diagonal) + root[:, None] * noise * root[None, :]


def draw_block_inverse(key, part):
    bounds = (0.5, 2.0)

    def one_block(index):
        block = symmetric_block(jax.random.fold_in(jax.random.fold_in(key, 11), index), B, bounds[0], bounds[1], 0.35)
        return block.astype(jnp.bfloat16)
    flat = lax.map(one_block, jnp.arange(GROUPS * WEEKS, dtype=jnp.int32))
    return flat.reshape(GROUPS, WEEKS, B, B)


def draw_shared_inverse(key, part):
    bounds = (0.82, 0.92)
    spread = 0.05

    def one_week(index):
        week_key = jax.random.fold_in(jax.random.fold_in(key, 23), index)
        first_key, second_key = jax.random.split(week_key)
        diagonal = jax.random.uniform(first_key, (SHARED,), jnp.float32, bounds[0], bounds[1])
        noise = jax.random.normal(second_key, (SHARED, SHARED), jnp.float32)
        noise = jnp.clip((noise + noise.T) * 0.7071067811865476, -4.0, 4.0) * (spread / jnp.sqrt(1.0 * SHARED))
        return jnp.diag(diagonal) + noise
    return lax.map(one_week, jnp.arange(WEEKS, dtype=jnp.int32))


def with_ends(array, rng, least, top_value):
    index_at = [jax.random.randint(jax.random.fold_in(rng, axis), (), 0, length) for axis, length in enumerate(array.shape)]
    main_axis = array.shape.index(max(array.shape))
    next_to = index_at[:main_axis] + [(index_at[main_axis] + 1) % array.shape[main_axis]] + index_at[main_axis + 1:]
    return array.at[tuple(index_at)].set(least).at[tuple(next_to)].set(top_value)


def block_levels(key, dims, cuts, low, high):
    gain, own = 1.0, jax.random.fold_in(key, 6)
    for dim, shards_of in cuts:
        steps = jnp.exp(jax.random.uniform(jax.random.fold_in(own, dim), (shards_of,), jnp.float32, low / len(cuts), high / len(cuts)))
        gain = gain * jnp.repeat(steps, dims[dim] // shards_of).reshape([-1 if axis == dim else 1 for axis in range(len(dims))])
    return gain


def centred(own_key, extent, width, reach, cuts=(), kind=jnp.bfloat16):
    loudness = block_levels(own_key, extent, cuts, -0.22, 0.18) if cuts else 1.0
    entries = jax.random.normal(own_key, extent, jnp.float32) * width * loudness
    return jnp.minimum(jnp.maximum(entries, -reach), reach).astype(kind)


def setup_inputs(seed: int = 0) -> dict:
    arg_keys = jax.random.split(jax.random.key(seed), 8)
    block_inverse = draw_block_inverse(jax.random.fold_in(arg_keys[7], 71), 0)
    coupling = centred(arg_keys[1], (GROUPS, WEEKS, B, SHARED), (8 * B) ** -0.5, 0.0390625, ((0, 4), (1, 16), (2, 2)))
    data_rhs = centred(arg_keys[2], (GROUPS, WEEKS, B, SAMPLES), 1.0, 6.0, ((0, 4), (1, 16), (2, 2)))
    station_seen = with_ends((jax.random.randint(arg_keys[3], (GROUPS, WEEKS, STATIONS), 0, 4) < 3).astype(jnp.int32), jax.random.fold_in(arg_keys[3], 1), 0, 1)
    shared_inverse = draw_shared_inverse(jax.random.fold_in(arg_keys[7], 71), 0)
    walk_weight = jnp.clip(jnp.exp(jax.random.uniform(arg_keys[5], (SHARED,), jnp.float32, math.log(0.92), math.log(1.0))), 0.92, 1.0)
    shared_rhs = centred(arg_keys[6], (WEEKS, SHARED, SAMPLES), 0.2, 1.2, ((0, 16),), jnp.float32)
    return {"block_inverse": block_inverse, "coupling": coupling, "data_rhs": data_rhs, "station_seen": station_seen, "shared_inverse": shared_inverse, "walk_weight": walk_weight, "shared_rhs": shared_rhs}


def reference(block_inverse, coupling, data_rhs, station_seen, shared_inverse, walk_weight, shared_rhs):
    blocks = GROUPS * WEEKS
    flat_inverse = block_inverse.reshape(blocks, B, B)
    flat_coupling = coupling.reshape(blocks, B, SHARED)
    flat_rhs = data_rhs.reshape(blocks, B, SAMPLES)
    flat_seen = jnp.repeat(station_seen, 3, axis=-1).astype(jnp.float32).reshape(blocks, B)
    step_matrix = shared_inverse * walk_weight[None, None, :]
    shared = jnp.zeros((WEEKS, SHARED, SAMPLES), jnp.float32)
    coords = jnp.zeros((blocks, B, SAMPLES), jnp.float32)
    for sweep_index in range(SWEEPS):
        later = jnp.concatenate([shared[1:], jnp.zeros((1, SHARED, SAMPLES), jnp.float32)], axis=0)
        shared_low = shared.astype(jnp.bfloat16)

        def solve_block(index):
            week = index % WEEKS
            product = jnp.dot(flat_coupling[index], shared_low[week], preferred_element_type=jnp.float32)
            residual_low = (flat_rhs[index].astype(jnp.float32) - product).astype(jnp.bfloat16)
            solved = flat_seen[index][:, None] * jnp.dot(flat_inverse[index], residual_low, preferred_element_type=jnp.float32)
            term = jnp.dot(flat_coupling[index].T, solved.astype(jnp.bfloat16), preferred_element_type=jnp.float32)
            return solved, term

        coords, terms = lax.map(solve_block, jnp.arange(blocks, dtype=jnp.int32))
        station_sum = terms.reshape(GROUPS, WEEKS, SHARED, SAMPLES).sum(axis=0)
        offsets = jnp.matmul(shared_inverse, shared_rhs + walk_weight[None, :, None] * later - station_sum, precision=lax.Precision.HIGHEST)

        def advance(previous, pieces):
            offset, matrix = pieces
            current = offset + jnp.dot(matrix, previous, precision=lax.Precision.HIGHEST)
            return current, current

        _, shared = lax.scan(advance, jnp.zeros((SHARED, SAMPLES), jnp.float32), (offsets, step_matrix))
    return coords.reshape(GROUPS, WEEKS, B, SAMPLES), shared
```

```python
import jax
import jax.numpy as jnp
from jax import lax
from jax.experimental.layout import Layout, with_layout_constraint
from jax.sharding import Mesh
from jax.sharding import PartitionSpec as P

CHAIN = ("chain_0", "chain_1", "chain_2")
AXES = ("chain_0", "chain_1", "chain_2", "tech", "blk")
SIZES = (4, 2, 2, 4, 2)
REPLICAS = ("tech", "blk")


def place(z, y, c, t, b):
    index = 0
    for value, size in zip((z, y, c, t, b), SIZES):
        index = index * size + value
    return index


def route(target_of):
    pairs = []
    for z in range(4):
        for y in range(2):
            for c in range(2):
                for t in range(4):
                    for b in range(2):
                        target = target_of(z, y, c, t, b)
                        if target is not None:
                            pairs.append((place(z, y, c, t, b), place(*target)))
    return pairs


BLK_SWAP = route(lambda z, y, c, t, b: (z, y, c, t, 1 - b))
CORE_SWAP = route(lambda z, y, c, t, b: (z, y, 1 - c, t, b))
CHIP_SWAP = route(lambda z, y, c, t, b: (z, 1 - y, c, t, b))
Z_HOPS = [
    route(lambda z, y, c, t, b, h=h: (h, y, c, t, b) if z == h - 1 else None) for h in (1, 2, 3)
]


def week_before(z, y, c, t, b):
    week = (z * 2 + y) * 2 + c - 1
    return None if week < 0 else (week // 4, week // 2 % 2, week % 2, t, b)


LATER = route(week_before)


def moved(value, pairs):
    return lax.ppermute(value, AXES, pairs)


def exact(left, right):
    return jnp.dot(left, right, precision=lax.Precision.HIGH)


def both_halves(own, other, which):
    rows = own.shape[0]
    whole = jnp.zeros((2 * rows, *own.shape[1:]), own.dtype)
    whole = lax.dynamic_update_slice_in_dim(whole, own, which * rows, 0)
    return lax.dynamic_update_slice_in_dim(whole, other, (1 - which) * rows, 0)


def collected(part):
    copies = jnp.broadcast_to(part, (8, *part.shape))
    pieces = lax.all_to_all(copies, REPLICAS, split_axis=0, concat_axis=0, tiled=True)
    return pieces.reshape(8 * part.shape[0], part.shape[1])


def row_major(value):
    return with_layout_constraint(value, Layout(major_to_minor=tuple(range(value.ndim))))


def layer(
    block_inverse, coupling, data_rhs, station_seen, shared_inverse, walk_weight, shared_rhs
):
    replica = lax.axis_index("tech") * 2 + lax.axis_index("blk")
    half = lax.axis_index("blk")
    early_chip = lax.axis_index("chain_1") == 0
    early_core = lax.axis_index("chain_2") == 0

    inverse_rows = block_inverse[0, 0]
    coupling_rows = coupling[0, 0]
    rhs_rows = data_rhs[0, 0]
    station_count = station_seen.shape[2]
    seen_rows = (
        jnp.broadcast_to(station_seen[0, 0][:, None], (station_count, 3))
        .reshape(-1, 1)
        .astype(jnp.float32)
    )
    inverse = shared_inverse[0]
    weight = walk_weight[None, :]
    samples = shared_rhs.shape[2] // 8
    week_rhs = lax.dynamic_slice_in_dim(shared_rhs[0].T, replica * samples, samples, 0)

    rhs_other = moved(rhs_rows, BLK_SWAP)

    step = walk_weight[:, None] * inverse
    step_other = moved(step, CORE_SWAP)
    step_first = jnp.where(early_core, step, step_other)
    step_second = jnp.where(early_core, step_other, step)
    pair = exact(step_first, step_second)
    own_map = jnp.where(early_core, step_first, pair)
    pair_other = moved(pair.astype(jnp.bfloat16), CHIP_SWAP)

    def solved(residual):
        return row_major(
            seen_rows * jnp.dot(inverse_rows, residual, preferred_element_type=jnp.float32)
        )

    def terms_of(coords):
        return lax.dot_general(
            coords.astype(jnp.bfloat16),
            coupling_rows,
            (((0,), (0,)), ((), ())),
            preferred_element_type=jnp.float32,
        ).astype(jnp.bfloat16)

    def summed(terms):
        pieces = lax.all_to_all(
            terms.reshape(8, samples, terms.shape[1]),
            REPLICAS,
            split_axis=0,
            concat_axis=0,
            tiled=True,
        )
        return jnp.sum(pieces.astype(jnp.float32), axis=0)

    def left(rhs, factor, values):
        product = lax.dot_general(
            factor, values, (((1,), (1,)), ((), ())), preferred_element_type=jnp.float32
        )
        return (rhs.astype(jnp.float32) - product).astype(jnp.bfloat16)

    coords = solved(both_halves(rhs_rows, rhs_other, half))
    terms = terms_of(lax.optimization_barrier(coords))
    terms, week_rhs, pair, own_map, step_first, step_second, early_core, early_chip = (
        lax.optimization_barrier(
            (terms, week_rhs, pair, own_map, step_first, step_second, early_core, early_chip)
        )
    )
    station_sum = summed(terms)

    def late_maps(pair_other):
        pair_other = pair_other.astype(jnp.float32)
        pair_first = jnp.where(early_chip, pair, pair_other)
        pair_second = jnp.where(early_chip, pair_other, pair)
        return pair_first, pair_second, exact(pair_first, pair_second)

    def chain(offset, maps):
        pair_first, pair_second, group = maps
        offset_other = moved(offset, CORE_SWAP)
        first = jnp.where(early_core, offset, offset_other)
        second = jnp.where(early_core, offset_other, offset)
        chip_end = second + exact(first, step_second)
        chip_other = moved(chip_end, CHIP_SWAP)
        chip_first = jnp.where(early_chip, chip_end, chip_other)
        chip_second = jnp.where(early_chip, chip_other, chip_end)
        group_end = chip_second + exact(chip_first, pair_second)
        inside = jnp.where(
            early_chip,
            jnp.where(early_core, first, chip_first),
            jnp.where(early_core, first + exact(chip_first, step_first), group_end),
        )
        carried = jnp.zeros_like(offset)
        for hop in Z_HOPS:
            carried = carried + moved(group_end + exact(carried, group), hop)
        entering = jnp.where(early_chip, carried, exact(carried, pair_first))
        return inside + exact(entering, own_map)

    pair_other, station_sum = lax.optimization_barrier((pair_other, station_sum))
    maps = late_maps(pair_other)
    shared = chain(exact(week_rhs - station_sum, inverse), maps)

    shared_low = shared.astype(jnp.bfloat16)
    shared_all = collected(shared_low)
    later = moved(shared_low, LATER).astype(jnp.float32)
    residual_own = left(rhs_rows, coupling_rows, shared_all)
    residual_other = moved(residual_own, BLK_SWAP)
    coords = solved(both_halves(residual_own, residual_other, half))
    station_sum = summed(terms_of(coords))
    shared = chain(exact(week_rhs + weight * later - station_sum, inverse), maps)
    result = collected(shared).T
    return (coords[None, None], result[None])


def solution(mesh):
    layout = Mesh(mesh.devices.reshape(SIZES), AXES)
    return jax.shard_map(
        layer,
        mesh=layout,
        in_specs=(
            P("tech", CHAIN, "blk", None),
            P("tech", CHAIN, "blk", None),
            P("tech", CHAIN, "blk", None),
            P("tech", CHAIN, "blk"),
            P(CHAIN, None, None),
            P(),
            P(CHAIN, None, None),
        ),
        out_specs=(P("tech", CHAIN, "blk", None), P(CHAIN, None, None)),
        check_vma=False,
    )
```

```python
import jax
import jax.numpy as jnp
from jax import lax
from jax.experimental.layout import Layout, with_layout_constraint
from jax.sharding import Mesh
from jax.sharding import PartitionSpec as P

CHAIN = ("chain_0", "chain_1", "chain_2")
AXES = ("chain_0", "chain_1", "chain_2", "tech", "blk")
SIZES = (4, 2, 2, 4, 2)
REPLICAS = ("tech", "blk")


def place(z, y, c, t, b):
    index = 0
    for value, size in zip((z, y, c, t, b), SIZES):
        index = index * size + value
    return index


def route(target_of):
    pairs = []
    for z in range(4):
        for y in range(2):
            for c in range(2):
                for t in range(4):
                    for b in range(2):
                        target = target_of(z, y, c, t, b)
                        if target is not None:
                            pairs.append((place(z, y, c, t, b), place(*target)))
    return pairs


BLK_SWAP = route(lambda z, y, c, t, b: (z, y, c, t, 1 - b))
CORE_SWAP = route(lambda z, y, c, t, b: (z, y, 1 - c, t, b))
CHIP_SWAP = route(lambda z, y, c, t, b: (z, 1 - y, c, t, b))
Z_HOPS = [
    route(lambda z, y, c, t, b, h=h: (h, y, c, t, b) if z == h - 1 else None) for h in (1, 2, 3)
]


def week_before(z, y, c, t, b):
    week = (z * 2 + y) * 2 + c - 1
    return None if week < 0 else (week // 4, week // 2 % 2, week % 2, t, b)


LATER = route(week_before)


def moved(value, pairs):
    return lax.ppermute(value, AXES, pairs)


def exact(left, right):
    return jnp.dot(left, right, precision=lax.Precision.HIGH)


def collected(part):
    copies = jnp.broadcast_to(part, (8, *part.shape))
    pieces = lax.all_to_all(copies, REPLICAS, split_axis=0, concat_axis=0, tiled=True)
    return pieces.reshape(8 * part.shape[0], part.shape[1])


def row_major(value):
    return with_layout_constraint(value, Layout(major_to_minor=tuple(range(value.ndim))))


def layer(
    block_inverse, coupling, data_rhs, station_seen, shared_inverse, walk_weight, shared_rhs
):
    replica = lax.axis_index("tech") * 2 + lax.axis_index("blk")
    half = lax.axis_index("blk")
    early_chip = lax.axis_index("chain_1") == 0
    early_core = lax.axis_index("chain_2") == 0

    inverse_rows = block_inverse[0, 0]
    coupling_rows = coupling[0, 0]
    rhs_rows = data_rhs[0, 0]
    station_count = station_seen.shape[2]
    seen_rows = (
        jnp.broadcast_to(station_seen[0, 0][:, None], (station_count, 3))
        .reshape(-1, 1)
        .astype(jnp.float32)
    )
    inverse = shared_inverse[0]
    weight = walk_weight[None, :]
    samples = shared_rhs.shape[2] // 8
    week_rhs = lax.dynamic_slice_in_dim(shared_rhs[0].T, replica * samples, samples, 0)

    rhs_other = moved(rhs_rows, BLK_SWAP)

    step = walk_weight[:, None] * inverse
    step_other = moved(step, CORE_SWAP)
    step_first = jnp.where(early_core, step, step_other)
    step_second = jnp.where(early_core, step_other, step)
    pair = exact(step_first, step_second)
    own_map = jnp.where(early_core, step_first, pair)
    pair_other = moved(pair.astype(jnp.bfloat16), CHIP_SWAP)

    def added(columns, rows):
        product = jnp.dot(columns, rows, preferred_element_type=jnp.float32)
        return lax.optimization_barrier(product)

    def solved(part, columns, rows):
        product = jnp.dot(columns, rows, preferred_element_type=jnp.float32)
        return row_major(seen_rows * (part + product))

    def terms_of(coords):
        return lax.dot_general(
            coords.astype(jnp.bfloat16),
            coupling_rows,
            (((0,), (0,)), ((), ())),
            preferred_element_type=jnp.float32,
        ).astype(jnp.bfloat16)

    def summed(terms):
        pieces = lax.all_to_all(
            terms.reshape(8, samples, terms.shape[1]),
            REPLICAS,
            split_axis=0,
            concat_axis=0,
            tiled=True,
        )
        return jnp.sum(pieces.astype(jnp.float32), axis=0)

    def left(rhs, factor, values):
        product = lax.dot_general(
            factor, values, (((1,), (1,)), ((), ())), preferred_element_type=jnp.float32
        )
        return (rhs.astype(jnp.float32) - product).astype(jnp.bfloat16)

    width = inverse_rows.shape[0]
    columns_own = lax.dynamic_slice_in_dim(inverse_rows, half * width, width, 1)
    columns_other = lax.dynamic_slice_in_dim(inverse_rows, (1 - half) * width, width, 1)
    columns_own, columns_other = lax.optimization_barrier((columns_own, columns_other))
    part = added(columns_own, rhs_rows)
    coords = solved(part, columns_other, rhs_other)
    terms = terms_of(lax.optimization_barrier(coords))
    terms, week_rhs, pair, own_map, step_first, step_second, early_core, early_chip = (
        lax.optimization_barrier(
            (terms, week_rhs, pair, own_map, step_first, step_second, early_core, early_chip)
        )
    )
    station_sum = summed(terms)

    def late_maps(pair_other):
        pair_other = pair_other.astype(jnp.float32)
        pair_first = jnp.where(early_chip, pair, pair_other)
        pair_second = jnp.where(early_chip, pair_other, pair)
        return pair_first, pair_second, exact(pair_first, pair_second)

    def chain(offset, maps):
        pair_first, pair_second, group = maps
        offset_other = moved(offset, CORE_SWAP)
        first = jnp.where(early_core, offset, offset_other)
        second = jnp.where(early_core, offset_other, offset)
        chip_end = second + exact(first, step_second)
        chip_other = moved(chip_end.astype(jnp.bfloat16), CHIP_SWAP).astype(jnp.float32)
        chip_first = jnp.where(early_chip, chip_end, chip_other)
        chip_second = jnp.where(early_chip, chip_other, chip_end)
        group_end = chip_second + exact(chip_first, pair_second)
        inside = jnp.where(
            early_chip,
            jnp.where(early_core, first, chip_first),
            jnp.where(early_core, first + exact(chip_first, step_first), group_end),
        )
        carried = jnp.zeros_like(offset)
        for hop in Z_HOPS:
            leaving = group_end + exact(carried, group)
            arrived = moved(leaving.astype(jnp.bfloat16), hop)
            carried = carried + arrived.astype(jnp.float32)
        entering = jnp.where(early_chip, carried, exact(carried, pair_first))
        return inside + exact(entering, own_map)

    pair_other, station_sum = lax.optimization_barrier((pair_other, station_sum))
    maps = late_maps(pair_other)
    shared = chain(exact(week_rhs - station_sum, inverse), maps)

    shared_low = shared.astype(jnp.bfloat16)
    shared_all = collected(shared_low)
    later = moved(shared_low, LATER).astype(jnp.float32)
    residual_own = row_major(left(rhs_rows, coupling_rows, shared_all))
    residual_other = moved(residual_own, BLK_SWAP)
    part = added(columns_own, residual_own)
    coords = solved(part, columns_other, residual_other)
    station_sum = summed(terms_of(coords))
    shared = chain(exact(week_rhs + weight * later - station_sum, inverse), maps)
    result = collected(shared.astype(jnp.bfloat16)).T.astype(jnp.float32)
    return (coords[None, None], result[None])


def solution(mesh):
    layout = Mesh(mesh.devices.reshape(SIZES), AXES)
    return jax.shard_map(
        layer,
        mesh=layout,
        in_specs=(
            P("tech", CHAIN, "blk", None),
            P("tech", CHAIN, "blk", None),
            P("tech", CHAIN, "blk", None),
            P("tech", CHAIN, "blk"),
            P(CHAIN, None, None),
            P(),
            P(CHAIN, None, None),
        ),
        out_specs=(P("tech", CHAIN, "blk", None), P(CHAIN, None, None)),
        check_vma=False,
    )
```

```python
import jax
import jax.numpy as jnp
from jax import lax
from jax.experimental.layout import Layout, with_layout_constraint
from jax.sharding import Mesh
from jax.sharding import PartitionSpec as P

CHAIN = ("chain_0", "chain_1", "chain_2")
AXES = ("chain_0", "chain_1", "chain_2", "tech", "blk")
SIZES = (4, 2, 2, 4, 2)
REPLICAS = ("tech", "blk")


def place(z, y, c, t, b):
    index = 0
    for value, size in zip((z, y, c, t, b), SIZES):
        index = index * size + value
    return index


def route(target_of):
    pairs = []
    for z in range(4):
        for y in range(2):
            for c in range(2):
                for t in range(4):
                    for b in range(2):
                        target = target_of(z, y, c, t, b)
                        if target is not None:
                            pairs.append((place(z, y, c, t, b), place(*target)))
    return pairs


BLK_SWAP = route(lambda z, y, c, t, b: (z, y, c, t, 1 - b))
CORE_SWAP = route(lambda z, y, c, t, b: (z, y, 1 - c, t, b))
CHIP_SWAP = route(lambda z, y, c, t, b: (z, 1 - y, c, t, b))
Z_HOPS = [
    route(lambda z, y, c, t, b, h=h: (h, y, c, t, b) if z == h - 1 else None) for h in (1, 2, 3)
]


def week_before(z, y, c, t, b):
    week = (z * 2 + y) * 2 + c - 1
    return None if week < 0 else (week // 4, week // 2 % 2, week % 2, t, b)


LATER = route(week_before)


def moved(value, pairs):
    return lax.ppermute(value, AXES, pairs)


def exact(left, right):
    return jnp.dot(left, right, precision=lax.Precision.HIGH)


def collected(part):
    copies = jnp.broadcast_to(part, (8, *part.shape))
    pieces = lax.all_to_all(copies, REPLICAS, split_axis=0, concat_axis=0, tiled=True)
    return pieces.reshape(8 * part.shape[0], part.shape[1])


def row_major(value):
    return with_layout_constraint(value, Layout(major_to_minor=tuple(range(value.ndim))))


def layer(
    block_inverse, coupling, data_rhs, station_seen, shared_inverse, walk_weight, shared_rhs
):
    replica = lax.axis_index("tech") * 2 + lax.axis_index("blk")
    half = lax.axis_index("blk")
    early_chip = lax.axis_index("chain_1") == 0
    early_core = lax.axis_index("chain_2") == 0

    inverse_rows = block_inverse[0, 0]
    coupling_rows = coupling[0, 0]
    rhs_rows = data_rhs[0, 0]
    station_count = station_seen.shape[2]
    seen_rows = (
        jnp.broadcast_to(station_seen[0, 0][:, None], (station_count, 3))
        .reshape(-1, 1)
        .astype(jnp.float32)
    )
    inverse = shared_inverse[0]
    weight = walk_weight[None, :]
    samples = shared_rhs.shape[2] // 8
    week_rhs = lax.dynamic_slice_in_dim(shared_rhs[0].T, replica * samples, samples, 0)

    rhs_other = moved(rhs_rows, BLK_SWAP)

    step = walk_weight[:, None] * inverse
    step_other = moved(step, CORE_SWAP)
    step_first = jnp.where(early_core, step, step_other)
    step_second = jnp.where(early_core, step_other, step)
    pair = exact(step_first, step_second)
    own_map = jnp.where(early_core, step_first, pair)
    half_size = pair.shape[0] // 2
    first_row = lax.axis_index("chain_2") * half_size
    sent = lax.dynamic_slice_in_dim(pair, first_row, half_size, 0)
    pair_got = moved(sent.astype(jnp.bfloat16), CHIP_SWAP)

    def added(columns, rows):
        product = jnp.dot(columns, rows, preferred_element_type=jnp.float32)
        return lax.optimization_barrier(product)

    def solved(part, columns, rows):
        product = jnp.dot(columns, rows, preferred_element_type=jnp.float32)
        return row_major(seen_rows * (part + product))

    def terms_of(coords):
        return lax.dot_general(
            coords.astype(jnp.bfloat16),
            coupling_rows,
            (((0,), (0,)), ((), ())),
            preferred_element_type=jnp.float32,
        ).astype(jnp.bfloat16)

    def summed(terms):
        pieces = lax.all_to_all(
            terms.reshape(8, samples, terms.shape[1]),
            REPLICAS,
            split_axis=0,
            concat_axis=0,
            tiled=True,
        )
        return jnp.sum(pieces.astype(jnp.float32), axis=0)

    early = coupling_rows.shape[0] // 3
    coupling_early = moved(coupling_rows[:early], BLK_SWAP)

    def left(rhs, factor, values):
        product = lax.dot_general(
            factor, values, (((1,), (1,)), ((), ())), preferred_element_type=jnp.float32
        )
        return (rhs.astype(jnp.float32) - product).astype(jnp.bfloat16)

    width = inverse_rows.shape[0]
    columns_own = lax.optimization_barrier(
        lax.dynamic_slice_in_dim(inverse_rows, half * width, width, 1)
    )
    part = added(columns_own, rhs_rows)
    inverse_rows, part = lax.optimization_barrier((inverse_rows, part))
    columns_other = lax.optimization_barrier(
        lax.dynamic_slice_in_dim(inverse_rows, (1 - half) * width, width, 1)
    )
    coords = solved(part, columns_other, rhs_other)
    terms = terms_of(lax.optimization_barrier(coords))
    terms, week_rhs, pair, own_map, step_first, step_second, early_core, early_chip = (
        lax.optimization_barrier(
            (terms, week_rhs, pair, own_map, step_first, step_second, early_core, early_chip)
        )
    )
    station_sum = summed(terms)

    def late_maps(pair_other):
        pair_other = pair_other.astype(jnp.float32)
        pair_first = jnp.where(early_chip, pair, pair_other)
        pair_second = jnp.where(early_chip, pair_other, pair)
        return pair_first, pair_second, exact(pair_first, pair_second)

    def chain(offset, maps):
        pair_first, pair_second, group = maps
        offset_other = moved(offset, CORE_SWAP)
        first = jnp.where(early_core, offset, offset_other)
        second = jnp.where(early_core, offset_other, offset)
        chip_end = second + exact(first, step_second)
        chip_other = moved(chip_end.astype(jnp.bfloat16), CHIP_SWAP).astype(jnp.float32)
        chip_first = jnp.where(early_chip, chip_end, chip_other)
        chip_second = jnp.where(early_chip, chip_other, chip_end)
        group_end = chip_second + exact(chip_first, pair_second)
        inside = jnp.where(
            early_chip,
            jnp.where(early_core, first, chip_first),
            jnp.where(early_core, first + exact(chip_first, step_first), group_end),
        )
        carried = jnp.zeros_like(offset)
        for hop in Z_HOPS:
            leaving = group_end + exact(carried, group)
            arrived = moved(leaving.astype(jnp.bfloat16), hop)
            carried = carried + arrived.astype(jnp.float32)
        entering = jnp.where(early_chip, carried, exact(carried, pair_first))
        return inside + exact(entering, own_map)

    pair_got, station_sum = lax.optimization_barrier((pair_got, station_sum))
    pair_rest = moved(pair_got, CORE_SWAP)
    pair_other = jnp.concatenate(
        [
            jnp.where(early_core, pair_got, pair_rest),
            jnp.where(early_core, pair_rest, pair_got),
        ]
    )
    maps = late_maps(pair_other)
    shared = chain(exact(week_rhs - station_sum, inverse), maps)

    shared_low = shared.astype(jnp.bfloat16)
    shared_all = collected(shared_low)
    later = moved(shared_low, LATER).astype(jnp.float32)
    residual_own = row_major(left(rhs_rows, coupling_rows, shared_all))
    residual_late = moved(row_major(residual_own[early:]), BLK_SWAP)
    residual_early = left(rhs_other[:early], coupling_early, shared_all)
    part = added(columns_own, residual_own)
    residual_other = jnp.concatenate([residual_early, residual_late])
    coords = solved(part, columns_other, residual_other)
    station_sum = summed(terms_of(coords))
    shared = chain(exact(week_rhs + weight * later - station_sum, inverse), maps)
    result = collected(shared.astype(jnp.bfloat16)).T.astype(jnp.float32)
    return (coords[None, None], result[None])


def solution(mesh):
    layout = Mesh(mesh.devices.reshape(SIZES), AXES)
    return jax.shard_map(
        layer,
        mesh=layout,
        in_specs=(
            P("tech", CHAIN, "blk", None),
            P("tech", CHAIN, "blk", None),
            P("tech", CHAIN, "blk", None),
            P("tech", CHAIN, "blk"),
            P(CHAIN, None, None),
            P(),
            P(CHAIN, None, None),
        ),
        out_specs=(P("tech", CHAIN, "blk", None), P(CHAIN, None, None)),
        check_vma=False,
    )
```

```python
import jax
import jax.numpy as jnp
from jax import lax
from jax.experimental.layout import Layout, with_layout_constraint
from jax.sharding import Mesh
from jax.sharding import PartitionSpec as P

CHAIN = ("chain_0", "chain_1", "chain_2")
AXES = ("chain_0", "chain_1", "chain_2", "tech", "blk")
SIZES = (4, 2, 2, 4, 2)
REPLICAS = ("tech", "blk")


def place(z, y, c, t, b):
    index = 0
    for value, size in zip((z, y, c, t, b), SIZES):
        index = index * size + value
    return index


def route(target_of):
    pairs = []
    for z in range(4):
        for y in range(2):
            for c in range(2):
                for t in range(4):
                    for b in range(2):
                        target = target_of(z, y, c, t, b)
                        if target is not None:
                            pairs.append((place(z, y, c, t, b), place(*target)))
    return pairs


BLK_SWAP = route(lambda z, y, c, t, b: (z, y, c, t, 1 - b))
CORE_SWAP = route(lambda z, y, c, t, b: (z, y, 1 - c, t, b))
CHIP_SWAP = route(lambda z, y, c, t, b: (z, 1 - y, c, t, b))
Z_HOPS = [
    route(lambda z, y, c, t, b, h=h: (h, y, c, t, b) if z == h - 1 else None) for h in (1, 2, 3)
]


def week_before(z, y, c, t, b):
    week = (z * 2 + y) * 2 + c - 1
    return None if week < 0 else (week // 4, week // 2 % 2, week % 2, t, b)


LATER = route(week_before)


def moved(value, pairs):
    return lax.ppermute(value, AXES, pairs)


def exact(left, right):
    return jnp.dot(left, right, precision=lax.Precision.HIGH)


def collected(part):
    copies = jnp.broadcast_to(part, (8, *part.shape))
    pieces = lax.all_to_all(copies, REPLICAS, split_axis=0, concat_axis=0, tiled=True)
    return pieces.reshape(8 * part.shape[0], part.shape[1])


def row_major(value):
    return with_layout_constraint(value, Layout(major_to_minor=tuple(range(value.ndim))))


def layer(
    block_inverse, coupling, data_rhs, station_seen, shared_inverse, walk_weight, shared_rhs
):
    replica = lax.axis_index("tech") * 2 + lax.axis_index("blk")
    half = lax.axis_index("blk")
    early_chip = lax.axis_index("chain_1") == 0
    early_core = lax.axis_index("chain_2") == 0

    inverse_rows = block_inverse[0, 0]
    coupling_rows = coupling[0, 0]
    rhs_rows = data_rhs[0, 0]
    station_count = station_seen.shape[2]
    seen_rows = (
        jnp.broadcast_to(station_seen[0, 0][:, None], (station_count, 3))
        .reshape(-1, 1)
        .astype(jnp.float32)
    )
    inverse = shared_inverse[0]
    weight = walk_weight[None, :]
    samples = shared_rhs.shape[2] // 8
    week_rhs = lax.dynamic_slice_in_dim(shared_rhs[0].T, replica * samples, samples, 0)

    rhs_other = moved(rhs_rows, BLK_SWAP)

    step = walk_weight[:, None] * inverse
    step_other = moved(step, CORE_SWAP)
    step_first = jnp.where(early_core, step, step_other)
    step_second = jnp.where(early_core, step_other, step)
    pair = exact(step_first, step_second)
    own_map = jnp.where(early_core, step_first, pair)
    half_size = pair.shape[0] // 2
    first_row = lax.axis_index("chain_2") * half_size
    sent = lax.dynamic_slice_in_dim(pair, first_row, half_size, 0)
    pair_got = moved(sent.astype(jnp.bfloat16), CHIP_SWAP)

    def added(columns, rows):
        product = jnp.dot(columns, rows, preferred_element_type=jnp.float32)
        return lax.optimization_barrier(product)

    def solved(part, columns, rows):
        product = jnp.dot(columns, rows, preferred_element_type=jnp.float32)
        return row_major(seen_rows * (part + product))

    def terms_of(coords):
        return lax.dot_general(
            coords.astype(jnp.bfloat16),
            coupling_rows,
            (((0,), (0,)), ((), ())),
            preferred_element_type=jnp.float32,
        ).astype(jnp.bfloat16)

    def summed(terms):
        pieces = lax.all_to_all(
            terms.reshape(8, samples, terms.shape[1]),
            REPLICAS,
            split_axis=0,
            concat_axis=0,
            tiled=True,
        )
        return jnp.sum(pieces.astype(jnp.float32), axis=0)

    first_rows = coupling_rows.shape[0] // 8
    early = first_rows + coupling_rows.shape[0] // 3
    coupling_first = moved(coupling_rows[:first_rows], BLK_SWAP)
    coupling_next = moved(coupling_rows[first_rows:early], BLK_SWAP)

    def left(rhs, factor, values):
        product = lax.dot_general(
            factor, values, (((1,), (1,)), ((), ())), preferred_element_type=jnp.float32
        )
        return (rhs.astype(jnp.float32) - product).astype(jnp.bfloat16)

    width = inverse_rows.shape[0]
    columns_own = lax.dynamic_slice_in_dim(inverse_rows, half * width, width, 1)
    part = added(columns_own, rhs_rows)
    inverse_rows, part = lax.optimization_barrier((inverse_rows, part))
    columns_other = lax.optimization_barrier(
        lax.dynamic_slice_in_dim(inverse_rows, (1 - half) * width, width, 1)
    )
    coords = solved(part, columns_other, rhs_other)
    terms = terms_of(lax.optimization_barrier(coords))
    terms, week_rhs, pair, own_map, step_first, step_second, early_core, early_chip = (
        lax.optimization_barrier(
            (terms, week_rhs, pair, own_map, step_first, step_second, early_core, early_chip)
        )
    )
    station_sum = summed(terms)

    def late_maps(pair_other):
        pair_other = pair_other.astype(jnp.float32)
        pair_first = jnp.where(early_chip, pair, pair_other)
        pair_second = jnp.where(early_chip, pair_other, pair)
        return pair_first, pair_second, exact(pair_first, pair_second)

    def chain(offset, maps):
        pair_first, pair_second, group = maps
        offset_other = moved(offset, CORE_SWAP)
        first = jnp.where(early_core, offset, offset_other)
        second = jnp.where(early_core, offset_other, offset)
        chip_end = second + exact(first, step_second)
        chip_other = moved(chip_end.astype(jnp.bfloat16), CHIP_SWAP).astype(jnp.float32)
        chip_first = jnp.where(early_chip, chip_end, chip_other)
        chip_second = jnp.where(early_chip, chip_other, chip_end)
        group_end = chip_second + exact(chip_first, pair_second)
        inside = jnp.where(
            early_chip,
            jnp.where(early_core, first, chip_first),
            jnp.where(early_core, first + exact(chip_first, step_first), group_end),
        )
        carried = jnp.zeros_like(offset)
        for hop in Z_HOPS:
            leaving = group_end + exact(carried, group)
            arrived = moved(leaving.astype(jnp.bfloat16), hop)
            carried = carried + arrived.astype(jnp.float32)
        entering = jnp.where(early_chip, carried, exact(carried, pair_first))
        return inside + exact(entering, own_map)

    pair_got, station_sum = lax.optimization_barrier((pair_got, station_sum))
    pair_rest = moved(pair_got, CORE_SWAP)
    pair_other = jnp.concatenate(
        [
            jnp.where(early_core, pair_got, pair_rest),
            jnp.where(early_core, pair_rest, pair_got),
        ]
    )
    maps = late_maps(pair_other)
    shared = chain(exact(week_rhs - station_sum, inverse), maps)

    shared_low = shared.astype(jnp.bfloat16)
    shared_all = collected(shared_low)
    later = moved(shared_low, LATER).astype(jnp.float32)
    residual_own = row_major(left(rhs_rows, coupling_rows, shared_all))
    residual_late = moved(row_major(residual_own[early:]), BLK_SWAP)
    coupling_early = jnp.concatenate([coupling_first, coupling_next])
    residual_early = left(rhs_other[:early], coupling_early, shared_all)
    part = added(columns_own, residual_own)
    residual_other = jnp.concatenate([residual_early, residual_late])
    coords = solved(part, columns_other, residual_other)
    station_sum = summed(terms_of(coords))
    shared = chain(exact(week_rhs + weight * later - station_sum, inverse), maps)
    result = collected(shared.astype(jnp.bfloat16)).T.astype(jnp.float32)
    return (coords[None, None], result[None])


def solution(mesh):
    layout = Mesh(mesh.devices.reshape(SIZES), AXES)
    return jax.shard_map(
        layer,
        mesh=layout,
        in_specs=(
            P("tech", CHAIN, "blk", None),
            P("tech", CHAIN, "blk", None),
            P("tech", CHAIN, "blk", None),
            P("tech", CHAIN, "blk"),
            P(CHAIN, None, None),
            P(),
            P(CHAIN, None, None),
        ),
        out_specs=(P("tech", CHAIN, "blk", None), P(CHAIN, None, None)),
        check_vma=False,
    )
```
